128 devices in a mesh: tm: 64 (over z, y, x), state: 2 (over core).
Axes of the slice: x: 4, y: 4, z: 4, core: 2. Of those that a mesh axis runs over, the one named last changes fastest.
Arguments:
- symbols: int32 [8], P('state'), may hold values from 0 to 255
- emission: float32 [8192, 256], P('tm'), may hold values from 0.2 to 5
- decay: float32 [2, 8192], P('state', 'tm'), may hold values from 0.05 to 1
- left_factor: float32 [2, 64, 8192], P('state', None, 'tm'), may hold values from 0.1 to 3
- right_factor: float32 [2, 64, 8192], P('state', None, 'tm'), may hold values from 0.001 to 0.03
- initial: float32 [8192], P('tm'), may hold values from 0.1 to 10
Outputs:
- filtered: float32 [8, 8192], P('state', 'tm')
- log_scale: float32 [8], P('state')
The draws below stay inside these ranges and needn't reach their ends.
All inputs are finite; a program needn't handle non-finite values.
Results may differ from the reference program's by a relative error of at most 0.00011.
Values sent between devices are 32-bit elements; how exact they have to be, the bound alone decides.
A program may use at most 64 MiB of HBM per device.

```python
import math
import jax
import jax.numpy as jnp
from jax import lax

S = 8192
R = 64
NSYM = 256
F_DEV = 4
SPANS = 2
FRAMES = 8
N_STATE = 2


def plant(entries, own_key, least, top_value):
    dims = entries.shape
    index_at = [jax.random.randint(jax.random.fold_in(own_key, axis), (), 0, dims[axis]) for axis in range(len(dims))]
    entries = entries.at[tuple(index_at)].set(least)
    longest = dims.index(max(dims))
    index_at[longest] = (index_at[longest] + 1) % dims[longest]
    return entries.at[tuple(index_at)].set(top_value)


def level_of(rng, shape, pieces, least, largest):
    loudness, own = 1.0, jax.random.fold_in(rng, 6)
    for position, parts in pieces:
        steps = jnp.exp(jax.random.uniform(jax.random.fold_in(own, position), (parts,), jnp.float32, least / len(pieces), largest / len(pieces)))
        loudness = loudness * jnp.repeat(steps, shape[position] // parts).reshape([-1 if axis == position else 1 for axis in range(len(shape))])
    return loudness


def setup_inputs(seed: int = 0) -> dict:
    keys = jax.random.split(jax.random.key(seed), 7)
    symbols = plant(jax.random.randint(keys[0], (FRAMES,), 0, NSYM), jax.random.fold_in(keys[0], 1), 0, NSYM - 1).astype(jnp.int32)
    emission = jnp.clip(jnp.exp(math.log(5.0) - 3.218876 * jax.random.uniform(keys[1], (S, NSYM), jnp.float32) ** level_of(keys[1], (S, NSYM), ((0, 64),), -0.2, 0.2)), 0.2, 5.0)
    decay = jnp.clip(jnp.exp(math.log(1.0) - 2.9957323 * jax.random.uniform(keys[2], (SPANS, S), jnp.float32) ** level_of(keys[2], (SPANS, S), ((0, 2), (1, 64)), -0.2, 0.2)), 0.05, 1.0)
    left_factor = jnp.clip(jnp.exp(math.log(3.0) - 3.4011974 * jax.random.uniform(keys[3], (SPANS, R, S), jnp.float32) ** level_of(keys[3], (SPANS, R, S), ((0, 2), (2, 64)), -0.2, 0.2)), 0.1, 3.0)
    right_factor = jnp.clip(jnp.exp(math.log(0.03) - 3.4011973 * jax.random.uniform(keys[4], (SPANS, R, S), jnp.float32) ** level_of(keys[4], (SPANS, R, S), ((0, 2), (2, 64)), -0.2, 0.2)), 0.001, 0.03)
    initial = jnp.clip(jnp.exp(math.log(10.0) - 4.6051702 * jax.random.uniform(keys[5], (S,), jnp.float32) ** level_of(keys[5], (S,), ((0, 64),), -0.2, 0.2)), 0.1, 10.0)
    return {"symbols": symbols, "emission": emission, "decay": decay, "left_factor": left_factor, "right_factor": right_factor, "initial": initial}


PRECISE = lax.Precision.HIGHEST


def reference(symbols, emission, decay, left_factor, right_factor, initial):
    belief_init = initial / jnp.mean(initial)

    def block(belief, inputs):
        symbol_row, decay_row, left_rows, right_rows = inputs

        def frame(belief_now, symbol):
            emitted = lax.dynamic_index_in_dim(emission, symbol, 1, keepdims=False)
            mixture = jnp.dot(left_rows, belief_now, precision=PRECISE) / S
            unscaled = emitted * (decay_row * belief_now + jnp.dot(mixture, right_rows, precision=PRECISE))
            normal = jnp.sum(unscaled) / S
            belief_next = unscaled / normal
            return belief_next, (belief_next, jnp.log(normal))

        return lax.scan(frame, belief, symbol_row)

    closing, (beliefs, log_levels) = lax.scan(block, belief_init, (symbols.reshape(N_STATE, F_DEV), decay, left_factor, right_factor))
    return beliefs.reshape(N_STATE * F_DEV, S), log_levels.reshape(N_STATE * F_DEV)
```

```python
import functools

import jax
import jax.numpy as jnp
from jax import lax
from jax.experimental import pallas as pl
from jax.experimental.pallas import tpu as pltpu
from jax.sharding import PartitionSpec as P

MESH = pl.DeviceIdType.MESH
PRECISE = lax.Precision.HIGHEST
LANES = 128
R = 64
F = 4
ROWS = 8 * R


def nt(a, b):
    return lax.dot_general(
        a, b, (((1,), (1,)), ((), ())), precision=PRECISE, preferred_element_type=jnp.float32
    )


def nn(a, b):
    return jnp.dot(a, b, precision=PRECISE, preferred_element_type=jnp.float32)


def iota(shape, axis):
    return lax.broadcasted_iota(jnp.int32, shape, axis)


def chain(e, d):
    p = [jnp.ones_like(d)]
    for r in range(F):
        p.append(p[-1] * (e[r : r + 1] * d))
    return p, [1.0 / (p[s] * d) for s in range(F)]


def kernel(
    dims,
    states,
    sym_hbm,
    emis_hbm,
    decay_hbm,
    left_hbm,
    right_hbm,
    init_hbm,
    out_ref,
    log_ref,
    sym,
    emis,
    dec,
    uv,
    init,
    other,
    emit,
    emit_other,
    part,
    rs_buf,
    line_src,
    line_buf,
    whole_src,
    whole,
    in_sem,
    send_sem,
    recv_sem,
):
    nz, ny, nx = dims
    plane = ny * nx
    piece = ROWS // plane
    tm = lax.axis_index("tm")
    core = lax.axis_index("state")
    x = lax.rem(tm, nx)
    y = lax.rem(lax.div(tm, nx), ny)
    z = lax.div(tm, plane)
    mine = y * nx + x

    def plane_peer(k):
        yy = lax.rem(y + k // nx, ny)
        xx = lax.rem(x + k % nx, nx)
        place = yy * nx + xx
        return place, z * plane + place

    def line_peer(k):
        return lax.rem(z + k, nz) * plane + mine

    barrier = pltpu.get_barrier_semaphore()

    def hail(target, on):
        pl.semaphore_signal(barrier, inc=1, device_id=(target, on), device_id_type=MESH)

    loads = [
        pltpu.make_async_copy(sym_hbm, sym, in_sem.at[0]),
        pltpu.make_async_copy(emis_hbm, emis, in_sem.at[1]),
        pltpu.make_async_copy(decay_hbm, dec, in_sem.at[2]),
        pltpu.make_async_copy(left_hbm.at[0], uv.at[0], in_sem.at[3]),
        pltpu.make_async_copy(right_hbm.at[0], uv.at[1], in_sem.at[4]),
        pltpu.make_async_copy(init_hbm, init, in_sem.at[5]),
    ]
    for load in loads:
        load.start()
    hail(tm, 1 - core)
    for k in range(1, plane):
        for on in range(2):
            hail(plane_peer(k)[1], on)
    for k in range(1, nz):
        hail(line_peer(k), core)
    for load in loads:
        load.wait()

    rows8 = iota((8, 256), 0)
    wanted = jnp.full((8, 256), -1, jnp.int32)
    for r in range(F):
        wanted = jnp.where(rows8 == r, sym[r], wanted)
    onehot = jnp.where(iota((8, 256), 1) == wanted, 1.0, 0.0)
    emitted = nt(onehot, emis[...])
    emit[...] = jnp.where(iota((8, LANES), 0) == F, dec[...], emitted)
    pl.semaphore_wait(barrier, 2 * (plane - 1) + nz)

    swaps = [
        pltpu.make_async_remote_copy(
            src_ref=uv.at[1 - core],
            dst_ref=other,
            send_sem=send_sem.at[0],
            recv_sem=recv_sem.at[0],
            device_id=(tm, 1 - core),
            device_id_type=MESH,
        ),
        pltpu.make_async_remote_copy(
            src_ref=emit,
            dst_ref=emit_other,
            send_sem=send_sem.at[1],
            recv_sem=recv_sem.at[1],
            device_id=(tm, 1 - core),
            device_id_type=MESH,
        ),
    ]
    for swap in swaps:
        swap.start()
    for swap in swaps:
        swap.wait()

    first = core == 0
    u_own = uv[0] * (1.0 / states)
    v_own = uv[1]
    u_hi = jnp.where(first, other[...], uv[0]) * (1.0 / states)
    v_lo = jnp.where(first, uv[1], other[...])
    e_own = emit[...]
    e_lo = jnp.where(first, emit[...], emit_other[...])
    e_hi = jnp.where(first, emit_other[...], emit[...])
    p_own, w_own = chain(e_own, e_own[F : F + 1])
    p_lo, w_lo = chain(e_lo, e_lo[F : F + 1])
    p_hi, w_hi = chain(e_hi, e_hi[F : F + 1])
    p_all = p_lo + [p_lo[F] * p_hi[r] for r in range(1, F + 1)]
    beta0 = init[...].reshape(1, LANES)

    zero = jnp.zeros((1, LANES), jnp.float32)
    tail = [jnp.where(first, p_all[t], zero) for t in range(F + 1, 2 * F + 1)]
    p_rows = jnp.concatenate(p_own[1:] + tail, axis=0)
    t_of_row = iota((8, LANES), 0) + 1
    quota = [
        jnp.where(t_of_row > s, p_rows * (e_own[F : F + 1] * w_own[s]), 0.0) for s in range(F)
    ]
    right0 = jnp.concatenate(quota + [jnp.zeros((R - 8 * F, LANES), jnp.float32), u_own * p_own[1]])
    part[0:R, :] = nt(v_own * w_own[0], right0)
    right1 = jnp.concatenate([u_own * p_own[2], u_own * p_own[3]])
    part[R : 4 * R, :] = nt(jnp.concatenate([v_own * w_own[s] for s in range(3)]), right1)
    p_a = p_all[F] * jnp.where(first, p_hi[0], p_hi[2])
    p_b = p_all[F] * jnp.where(first, p_hi[1], p_hi[3])
    right2 = jnp.concatenate([u_hi * p_a, u_hi * p_b])
    part[4 * R :, :] = nt(jnp.concatenate([v_lo * w_lo[s] for s in range(F)]), right2)

    starts = jnp.concatenate([p * beta0 for p in p_all] + [jnp.zeros((7, LANES), jnp.float32)])
    led = nt(starts[:8], jnp.concatenate([u_own, u_hi]))
    led = jnp.where(iota((8, LANES), 0) < F, led, pltpu.roll(led, R, 1))
    sums = jnp.broadcast_to(jnp.sum(starts, axis=1, keepdims=True), (16, LANES))
    low = iota((8, LANES), 1) < R
    part[3 * R : 3 * R + 8, :] = jnp.where(low, led, part[3 * R : 3 * R + 8, :])
    low16 = iota((16, LANES), 1) < R
    part[3 * R + 16 : 3 * R + 32, :] = jnp.where(low16, sums, part[3 * R + 16 : 3 * R + 32, :])

    def at_piece(p):
        return pl.ds(pl.multiple_of(p * piece, piece), piece)

    for k in range(1, plane):
        place, chip = plane_peer(k)
        pltpu.make_async_remote_copy(
            src_ref=part.at[at_piece(place)],
            dst_ref=rs_buf.at[k - 1],
            send_sem=send_sem.at[2],
            recv_sem=recv_sem.at[2],
            device_id=(chip, core),
            device_id_type=MESH,
        ).start()
    drain = pltpu.make_async_remote_copy(
        src_ref=rs_buf,
        dst_ref=rs_buf,
        send_sem=send_sem.at[2],
        recv_sem=recv_sem.at[2],
        device_id=(tm, 1 - core),
        device_id_type=MESH,
    )
    drain.wait_recv()
    total = part[at_piece(mine), :]
    for k in range(plane - 1):
        total = total + rs_buf[k]
    line_src[...] = total

    for k in range(1, nz):
        pltpu.make_async_remote_copy(
            src_ref=line_src,
            dst_ref=line_buf.at[k - 1],
            send_sem=send_sem.at[3],
            recv_sem=recv_sem.at[3],
            device_id=(line_peer(k), core),
            device_id_type=MESH,
        ).start()
    line_drain = pltpu.make_async_remote_copy(
        src_ref=line_buf,
        dst_ref=line_buf,
        send_sem=send_sem.at[3],
        recv_sem=recv_sem.at[3],
        device_id=(tm, 1 - core),
        device_id_type=MESH,
    )
    line_drain.wait_recv()
    for k in range(nz - 1):
        total = total + line_buf[k]
    whole_src[...] = total
    here = pl.ds(pl.multiple_of(core * ROWS + mine * piece, piece), piece)
    whole[here, :] = total

    def give(chip, on):
        pltpu.make_async_remote_copy(
            src_ref=whole_src,
            dst_ref=whole.at[here],
            send_sem=send_sem.at[4],
            recv_sem=recv_sem.at[4],
            device_id=(chip, on),
            device_id_type=MESH,
        ).start()

    for k in range(1, plane):
        give(plane_peer(k)[1], 1)
    early = jnp.logical_and(first, mine < plane // 2)

    @pl.when(first)
    def _():
        give(tm, 1)

    @pl.when(early)
    def _():
        for k in range(1, plane):
            give(plane_peer(k)[1], 0)

    def taken(rows):
        return pltpu.make_async_remote_copy(
            src_ref=whole.at[pl.ds(0, rows)],
            dst_ref=whole.at[pl.ds(0, rows)],
            send_sem=send_sem.at[4],
            recv_sem=recv_sem.at[4],
            device_id=(tm, 1 - core),
            device_id_type=MESH,
        )

    @pl.when(jnp.logical_not(first))
    def _():
        taken((2 * plane - 1) * piece).wait_recv()

    @pl.when(early)
    def _():
        taken((plane // 2 - 1) * piece).wait_recv()

    @pl.when(jnp.logical_and(first, mine >= plane // 2))
    def _():
        taken((plane // 2) * piece).wait_recv()

    lane8 = iota((8, LANES), 1)
    row8 = iota((8, LANES), 0)
    high = lane8 >= R

    def pair(base, q):
        a0 = whole[base + 2 * q : base + 2 * q + 1, :]
        a1 = whole[base + 2 * q + 1 : base + 2 * q + 2, :]
        a0 = jnp.broadcast_to(a0, (8, LANES))
        a1 = pltpu.roll(jnp.broadcast_to(a1, (8, LANES)), R, 1)
        return jnp.where(high, a1, a0)

    def close(a, top):
        return a + jnp.where(high, nn(a[:, :R], whole[top : top + R, :]), 0.0)

    def spread(xs, at):
        rows = jnp.zeros((8, LANES), jnp.float32)
        for q, xq in enumerate(xs):
            for h in range(2):
                keep = jnp.logical_and(row8 == at + 2 * q + h, high == (h == 1))
                rows = jnp.where(keep, xq, rows)
        return rows

    def twice(a):
        return jnp.concatenate([a, a], axis=0)

    E_AT = 3 * R
    x0 = close(pair(E_AT, 0), 0)
    x1 = close(pair(E_AT, 1) + nn(x0, whole[R : 3 * R, :]), 3 * R)
    rows_lo = spread([x0, x1], 0)
    y_lo = nn(rows_lo, twice(v_lo))
    tally_lo = nn(rows_lo, twice(whole[0:R, :]))

    def start_sum(t):
        return whole[E_AT + 16 + t : E_AT + 17 + t, 0:1]

    def tally(table, t):
        keep = jnp.logical_and(lane8 == 8 * row8 + (t - 1), row8 < F)
        return jnp.sum(jnp.where(keep, table, 0.0), keepdims=True)

    def finish(gamma, y, w, p, sums):
        for r in range(F):
            gamma = gamma + w[r] * y[r : r + 1]
            out_ref[r : r + 1, :] = p[r] * gamma * (states / sums[r + 1])
            log_ref[r : r + 1, :] = jnp.broadcast_to(jnp.log(sums[r + 1] / sums[r]), (1, LANES))
        log_ref[F:8, :] = jnp.zeros((8 - F, LANES), jnp.float32)

    @pl.when(first)
    def _():
        sums = [start_sum(0)] + [start_sum(t) + tally(tally_lo, t) for t in range(1, F + 1)]
        finish(beta0, y_lo, w_lo, p_all[1 : F + 1], sums)

    @pl.when(jnp.logical_not(first))
    def _():
        c0, c1 = (ROWS + k * R for k in (0, 3))
        x2 = pair(E_AT, 2) + nn(x0, whole[4 * R : 6 * R, :]) + nn(x1, whole[6 * R : 8 * R, :])
        x2 = close(x2, c0)
        x3 = pair(E_AT, 3) + nn(x0, whole[ROWS + 4 * R : ROWS + 6 * R, :])
        x3 = x3 + nn(x1, whole[ROWS + 6 * R : ROWS + 8 * R, :])
        x3 = close(x3 + nn(x2, whole[ROWS + R : ROWS + 3 * R, :]), c1)
        rows_hi = spread([x2, x3], 0)
        y_hi = nn(rows_hi, twice(v_own))
        tally_hi = nn(rows_hi, twice(whole[c0 : c0 + R, :]))
        sums = [start_sum(F) + tally(tally_lo, F)]
        for t in range(1, F + 1):
            sums.append(start_sum(F + t) + tally(tally_lo, F + t) + tally(tally_hi, t))
        gamma = beta0
        for r in range(F):
            gamma = gamma + w_lo[r] * y_lo[r : r + 1]
        w = [w_hi[r] / p_lo[F] for r in range(F)]
        finish(gamma, y_hi, w, p_all[F + 1 :], sums)

    drain.wait_send()
    line_drain.wait_send()
    taken((plane - 1) * piece).wait_send()

    @pl.when(first)
    def _():
        taken(piece).wait_send()

    @pl.when(early)
    def _():
        taken((plane - 1) * piece).wait_send()


def solution(mesh, dims=(4, 4, 4)):
    states = LANES * mesh.shape["tm"]
    plane = dims[1] * dims[2]
    piece = ROWS // plane

    def per_device(symbols, emission, decay, left_factor, right_factor, initial):
        f32 = jnp.float32
        filtered, logs = pl.pallas_call(
            functools.partial(kernel, dims, states),
            out_shape=(
                jax.ShapeDtypeStruct((F, LANES), f32),
                jax.ShapeDtypeStruct((8, LANES), f32),
            ),
            in_specs=[pl.BlockSpec(memory_space=pl.ANY)] * 6,
            out_specs=(pl.BlockSpec(memory_space=pltpu.VMEM),) * 2,
            scratch_shapes=[
                pltpu.SMEM((F,), jnp.int32),
                pltpu.VMEM((LANES, 256), f32),
                pltpu.VMEM((1, LANES), f32),
                pltpu.VMEM((2, R, LANES), f32),
                pltpu.VMEM((LANES,), f32),
                pltpu.VMEM((R, LANES), f32),
                pltpu.VMEM((8, LANES), f32),
                pltpu.VMEM((8, LANES), f32),
                pltpu.VMEM((ROWS, LANES), f32),
                pltpu.VMEM((plane - 1, piece, LANES), f32),
                pltpu.VMEM((piece, LANES), f32),
                pltpu.VMEM((dims[0] - 1, piece, LANES), f32),
                pltpu.VMEM((piece, LANES), f32),
                pltpu.VMEM((2 * ROWS, LANES), f32),
                pltpu.SemaphoreType.DMA((6,)),
                pltpu.SemaphoreType.DMA((5,)),
                pltpu.SemaphoreType.DMA((5,)),
            ],
            compiler_params=pltpu.CompilerParams(collective_id=0, has_side_effects=True),
        )(symbols, emission, decay, left_factor, right_factor, initial)
        return filtered, logs[:F, 0]

    return jax.shard_map(
        per_device,
        mesh=mesh,
        in_specs=(
            P("state"),
            P("tm", None),
            P("state", "tm"),
            P("state", None, "tm"),
            P("state", None, "tm"),
            P("tm"),
        ),
        out_specs=(P("state", "tm"), P("state")),
        check_vma=False,
    )
```
